512 devices in a mesh: row: 32 (over z, core), col: 16 (over x, y).
Axes of the slice: x: 4, y: 4, z: 16, core: 2. Of those that a mesh axis runs over, the one named last changes fastest.
Arguments:
- view_left: bfloat16 [16384, 16384], P('row', 'col'), may hold values from -0.046875 to 0.046875
- view_right: bfloat16 [16384, 16384], P('row', 'col'), may hold values from -6 to 6
- view_product: bfloat16 [16384, 16384], P('row', 'col'), may hold values from -6 to 6
- delta_a_left: bfloat16 [16384, 512], P('row', 'col'), may hold values from -0.25 to 0.25
- delta_a_right: bfloat16 [16384, 512], P('row', 'col'), may hold values from -0.09375 to 0.09375
- delta_b_left: bfloat16 [16384, 512], P('col', 'row'), may hold values from -6 to 6
- delta_b_right: bfloat16 [16384, 512], P('col', 'row'), may hold values from -0.25 to 0.25
Outputs:
- updated_view: bfloat16 [16384, 16384], P('row', 'col')
The draws below stay inside these ranges and needn't reach their ends.
All inputs are finite; a program needn't handle non-finite values.
Results may differ from the reference program's by a relative error of at most 0.005.
Values may be sent and summed in bfloat16 or wider, within the bound.
A program may use at most 64 MiB of HBM per device.

```python
import jax
import jax.numpy as jnp

N = 16384
R = 512


def spiked(array, stream_key, source, target, blocks, factor):
    def block_of(position):
        return (jnp.arange(array.shape[position]) // (array.shape[position] // blocks)).reshape((-1,) + (1,) * (array.ndim - 1 - position))

    near = jax.random.permutation(stream_key, blocks)[block_of(target)]
    far = (block_of(target) + blocks // 2) % blocks
    return jnp.where((block_of(source) == near) | (block_of(source) == far), factor * array, array)


def block_scale(rng, dims, cuts, least, top_value):
    level = 1.0
    for dim, blocks in cuts:
        steps = jax.random.uniform(jax.random.fold_in(jax.random.fold_in(rng, 6), dim), (blocks,), jnp.float32, least / len(cuts), top_value / len(cuts))
        level = level * jnp.repeat(jnp.exp(steps), dims[dim] // blocks).reshape((-1,) + (1,) * (len(dims) - 1 - dim))
    return level


def noise(rng, shape, width, bound, cuts=(), held_as=jnp.bfloat16):
    values = jax.random.normal(rng, shape, jnp.float32) * width
    if len(cuts) > 0:
        values = block_scale(rng, shape, cuts, -0.22, 0.18) * values
    return jnp.clip(values, min=-bound, max=bound).astype(held_as)


def heavy_noise(own_key, dims, deviation, bound, split, heavy, kind=jnp.bfloat16):
    result = deviation * jax.random.normal(own_key, dims, jnp.float32)
    if split:
        result = result * block_scale(own_key, dims, split, -0.22, 0.18)
    return jnp.clip(spiked(result, jax.random.fold_in(own_key, 3), *heavy), -bound, bound).astype(kind)


def setup_inputs(seed: int = 0) -> dict:
    arg_keys = jax.random.split(jax.random.key(seed), 8)
    return {
        "view_left": noise(arg_keys[0], (N, N), N ** -0.5, 0.046875, ((0, 32), (1, 16))),
        "view_right": noise(arg_keys[1], (N, N), 1.0, 6.0, ((0, 32), (1, 16))),
        "view_product": noise(arg_keys[2], (N, N), 1.0, 6.0, ((0, 32), (1, 16))),
        "delta_a_left": noise(arg_keys[3], (N, R), R ** -0.5, 0.25, ((0, 32), (1, 16))),
        "delta_a_right": heavy_noise(arg_keys[4], (N, R), N ** -0.5, 0.09375, ((0, 32), (1, 16)), (0, 1, 32, 2.75)),
        "delta_b_left": noise(arg_keys[5], (N, R), 1.0, 6.0, ((0, 16), (1, 32))),
        "delta_b_right": noise(arg_keys[6], (N, R), R ** -0.5, 0.25, ((0, 16), (1, 32))),
    }


def reference(view_left, view_right, view_product, delta_a_left, delta_a_right, delta_b_left, delta_b_right):
    cross = jnp.dot(delta_a_right.T, delta_b_left, preferred_element_type=jnp.float32).astype(jnp.bfloat16)
    column_sum = jnp.dot(delta_a_right.T, view_right, preferred_element_type=jnp.float32)
    weights_w = (column_sum + jnp.dot(cross, delta_b_right.T, preferred_element_type=jnp.float32)).astype(jnp.bfloat16)
    projected = jnp.dot(view_left, delta_b_left, preferred_element_type=jnp.float32).astype(jnp.bfloat16)
    updated = view_product.astype(jnp.float32) + jnp.dot(delta_a_left, weights_w, preferred_element_type=jnp.float32)
    updated = updated + jnp.dot(projected, delta_b_right.T, preferred_element_type=jnp.float32)
    return updated.astype(jnp.bfloat16)
```

```python
import functools

import jax
import jax.numpy as jnp
from jax import lax
from jax.experimental import pallas as pl
from jax.experimental.pallas import tpu as pltpu
from jax.sharding import Mesh
from jax.sharding import PartitionSpec as P

MESH = pl.DeviceIdType.MESH
F32 = jnp.float32
BF16 = jnp.bfloat16
NZ = 16
HALF = 256
NT = (((1,), (1,)), ((), ()))


def rem(a, n):
    return lax.rem(a + 2 * n, n)


def kernel(
    vt_h, ut_h, pt_h, qt_h, a_h, b_h, c_h, out_h,
    PT, QT, VT, UT, U, A, B, C, OUT,
    WOWN, WSND, WRCV, RSP, RRP, RSM, RRM, WT,
    CS, CIN, CR, DF, DS, R1, EF, ES, R2, PJ, ACC,
    load_sem, psem, psnd, qsem, qsnd, wsem, wsnd, xrcv, xsnd,
    rpr, rps, rmr, rms, vsem, vsnd, usem, usnd, crsem, crsnd,
    dsem, dsnd, jsem, jsnd, cinsem, csnd,
):
    z = lax.axis_index("z")
    k = lax.axis_index("k")
    x = lax.axis_index("x")
    y = lax.axis_index("y")
    sib = {"k": 1 - k}
    zp, zm = {"z": rem(z + 1, NZ)}, {"z": rem(z - 1, NZ)}
    pos = {"x": x, "y": y}
    pending = []

    def send(src, dst, ssem, rsem, dev):
        copy = pltpu.make_async_remote_copy(
            src_ref=src, dst_ref=dst, send_sem=ssem, recv_sem=rsem,
            device_id=dev, device_id_type=MESH,
        )
        copy.start()
        pending.append(copy)

    def recv(dst, rsem):
        pltpu.make_async_remote_copy(
            src_ref=dst, dst_ref=dst, send_sem=rsem, recv_sem=rsem,
            device_id=sib, device_id_type=MESH,
        ).wait_recv()

    loads = [
        pltpu.make_async_copy(pt_h, PT.at[2 * z + k], load_sem.at[0]),
        pltpu.make_async_copy(vt_h, VT.at[x, y], load_sem.at[1]),
        pltpu.make_async_copy(qt_h, QT.at[2 * z + k], load_sem.at[2]),
        pltpu.make_async_copy(ut_h, UT.at[x, y], load_sem.at[3]),
        pltpu.make_async_copy(b_h, B, load_sem.at[4]),
        pltpu.make_async_copy(a_h, A, load_sem.at[5]),
        pltpu.make_async_copy(c_h, C, load_sem.at[6]),
    ]
    for copy in loads:
        copy.start()

    barrier = pltpu.get_barrier_semaphore()
    peers = [zp, zm, sib]
    for axis in ("x", "y"):
        for step in (1, 3, 2):
            peers.append({axis: rem(pos[axis] + step, 4)})
    for dev in peers:
        pl.semaphore_signal(barrier, inc=1, device_id=dev, device_id_type=MESH)
    pl.semaphore_wait(barrier, len(peers))

    class ZGather:
        def __init__(self, buf, rsem, ssem, slot):
            self.buf, self.rsem, self.ssem, self.slot = buf, rsem, ssem, slot
            self.n = 0

        def out(self, ref, rs, dev):
            send(ref, ref, self.ssem.at[self.n], self.rsem.at[rs], dev)
            self.n += 1

        def start(self):
            own = self.buf.at[self.slot(z, k)]
            self.out(own, 0, zp)
            self.out(own, 8, zm)
            self.out(own, 16, sib)

        def step(self, s):
            ref = self.buf.at[self.slot(rem(z - 1 - s, NZ), k)]
            recv(ref, self.rsem.at[s])
            if s < 7:
                self.out(ref, s + 1, zp)
            self.out(ref, 17 + s, sib)
            if s < 7:
                ref = self.buf.at[self.slot(rem(z + 1 + s, NZ), k)]
                recv(ref, self.rsem.at[8 + s])
                if s < 6:
                    self.out(ref, 9 + s, zm)
                self.out(ref, 25 + s, sib)

        def finish(self):
            recv(self.buf.at[self.slot(z, 1 - k)], self.rsem.at[16])
            for s in range(8):
                recv(self.buf.at[self.slot(rem(z - 1 - s, NZ), 1 - k)], self.rsem.at[17 + s])
                if s < 7:
                    recv(self.buf.at[self.slot(rem(z + 1 + s, NZ), 1 - k)], self.rsem.at[25 + s])

    class PlaneGather:
        def __init__(self, buf, lanes, first, rsem, ssem, base):
            self.buf, self.lanes, self.first = buf, lanes, first
            self.rsem, self.ssem, self.base = rsem, ssem, base

        def view(self, phase, at):
            if phase == 0:
                spot = {**pos, self.first: at}
                return self.buf.at[spot["x"], spot["y"], :, self.lanes]
            if self.first == "x":
                return self.buf.at[:, at, :, self.lanes]
            return self.buf.at[at, :, :, self.lanes]

        def start(self, phase):
            axis = self.first if phase == 0 else ("y" if self.first == "x" else "x")
            mine = self.view(phase, pos[axis])
            for i, step in enumerate((1, 3, 2)):
                at = self.base + 3 * phase + i
                send(mine, mine, self.ssem.at[at], self.rsem.at[at], {axis: rem(pos[axis] + step, 4)})

        def wait(self, phase):
            axis = self.first if phase == 0 else ("y" if self.first == "x" else "x")
            for i, step in enumerate((1, 3, 2)):
                at = self.base + 3 * phase + i
                recv(self.view(phase, rem(pos[axis] - step, 4)), self.rsem.at[at])

    lanes = [pl.ds(0, HALF), pl.ds(HALF, HALF)]
    order = ["x", "y"]

    def halves(buf, rsem, ssem):
        return [PlaneGather(buf, lanes[h], order[h], rsem, ssem, 6 * h) for h in (0, 1)]

    gp = ZGather(PT, psem, psnd, lambda zz, kk: 2 * zz + kk)
    gq = ZGather(QT, qsem, qsnd, lambda zz, kk: 2 * zz + kk)
    gw = ZGather(WT, wsem, wsnd, lambda zz, kk: 16 * kk + zz)
    gv = halves(VT, vsem, vsnd)
    gu = halves(UT, usem, usnd)
    gc = halves(CR, crsem, crsnd)
    gj = halves(PJ, jsem, jsnd)

    def both(gathers, what, phase):
        for g in gathers:
            getattr(g, what)(phase)

    def rs_step(s):
        d = rem(z + 8 - s, NZ)
        total = WOWN[d]
        if s > 0:
            recv(RRP.at[s - 1], rpr.at[s - 1])
            total = total + RRP[s - 1].astype(F32)
        RSP[s] = total.astype(BF16)
        send(RSP.at[s], RRP.at[s], rps.at[s], rpr.at[s], zp)
        if s < 7:
            d = rem(z - 7 + s, NZ)
            total = WOWN[d]
            if s > 0:
                recv(RRM.at[s - 1], rmr.at[s - 1])
                total = total + RRM[s - 1].astype(F32)
            RSM[s] = total.astype(BF16)
            send(RSM.at[s], RRM.at[s], rms.at[s], rmr.at[s], zm)

    loads[0].wait()
    gp.start()
    loads[1].wait()
    both(gv, "start", 0)
    loads[2].wait()
    gq.start()
    loads[3].wait()

    gp.step(0)
    gq.step(0)
    both(gv, "wait", 0)
    both(gv, "start", 1)
    both(gu, "start", 0)
    gp.step(1)
    gq.step(1)
    gp.step(2)
    gq.step(2)
    both(gv, "wait", 1)
    both(gu, "wait", 0)
    both(gu, "start", 1)
    loads[4].wait()

    def partial_w(dst, which):
        rows = VT[pl.ds(2 * which, 2)].reshape(HALF, 512)

        @pl.loop(0, 4)
        def _(j):
            at = pl.ds(pl.multiple_of(j * HALF, HALF), HALF)
            dst[:, :, at] = jnp.dot(rows, B[:, at], preferred_element_type=F32).reshape(NZ, 16, HALF)

    partial_w(WSND, 1 - k)
    send(WSND, WRCV, xsnd, xrcv, sib)
    partial_w(WOWN, k)
    gp.step(3)
    gq.step(3)
    recv(WRCV, xrcv)
    WOWN[...] = WOWN[...] + WRCV[...]
    rs_step(0)
    gp.step(4)
    gq.step(4)
    rs_step(1)
    both(gu, "wait", 1)
    U[...] = UT[...].reshape(512, 512).T
    gp.step(5)
    gq.step(5)
    rs_step(2)
    gp.step(6)
    gq.step(6)
    rs_step(3)
    gp.step(7)
    gp.finish()

    diag = z == 4 * x + y

    def cross_copy(d, kk, n):
        zz = rem(z + d, NZ)
        return pltpu.make_async_remote_copy(
            src_ref=CS.at[kk, zz], dst_ref=CIN.at[k], send_sem=csnd.at[n], recv_sem=cinsem.at[k],
            device_id={"z": zz, "k": kk}, device_id_type=MESH,
        )

    @pl.when(diag)
    def _():
        cols = pl.ds(pl.multiple_of(512 * k, 512), 512)
        rows = VT[...].reshape(512, 512)
        part = lax.dot_general(rows, PT[:, :, cols].reshape(512, 512), NT, preferred_element_type=F32)
        CS[...] = part.astype(BF16).reshape(2, NZ, 16, 512)
        n = 0
        for d in (8, 7, 9, 6, 10, 5, 11, 4, 12, 3, 13, 2, 14, 1, 15):
            for kk in (0, 1):
                cross_copy(d, kk, n).start()
                n += 1
        pltpu.make_async_remote_copy(
            src_ref=CS.at[1 - k, z], dst_ref=CIN.at[k], send_sem=csnd.at[n], recv_sem=cinsem.at[k],
            device_id=sib, device_id_type=MESH,
        ).start()
        CIN[k] = CS[k, z]

    gq.step(7)
    loads[5].wait()
    rs_step(4)

    points = PT[...].reshape(512, 1024)
    for i in range(4):
        part = lax.dot_general(A[pl.ds(128 * i, 128), :], points, NT, preferred_element_type=F32)
        part = part.reshape(4, 32, 512)
        DF[i] = part
        DS[i] = part.astype(BF16)

    def d_start(phase):
        for h in (0, 1):
            axis = order[h] if phase == 0 else order[1 - h]
            for i, step in enumerate((1, 3, 2)):
                t = rem(pos[axis] + step, 4)
                at = 6 * h + 3 * phase + i
                if phase == 1:
                    src, dst = ES.at[h, t], R2.at[h, i]
                else:
                    src = DS.at[t, :, :, lanes[h]] if h == 0 else DS.at[:, t, :, lanes[h]]
                    dst = R1.at[h, i]
                send(src, dst, dsnd.at[at], dsem.at[at], {axis: t})

    def d_first():
        for h in (0, 1):
            for i in range(3):
                recv(R1.at[h, i], dsem.at[6 * h + i])
            total = DF[x, :, :, lanes[h]] if h == 0 else DF[:, y, :, lanes[h]]
            for i in range(3):
                total = total + R1[h, i].astype(F32)
            EF[h] = total
            ES[h] = total.astype(BF16)
        d_start(1)

    def d_second():
        for h in (0, 1):
            for i in range(3):
                recv(R2.at[h, i], dsem.at[6 * h + 3 + i])
            total = EF[h, pos[order[1 - h]]]
            for i in range(3):
                total = total + R2[h, i].astype(F32)
            PJ[x, y, :, lanes[h]] = total.astype(BF16)

    d_start(0)
    rs_step(5)

    @pl.when(jnp.logical_not(diag))
    def _():
        for j in (0, 1):
            recv(CIN.at[j], cinsem.at[j])

    @pl.when(diag)
    def _():
        recv(CIN.at[1 - k], cinsem.at[1 - k])

    CR[x, y] = (CIN[0].astype(F32) + CIN[1].astype(F32)).astype(BF16)
    both(gc, "start", 0)
    rs_step(6)
    d_first()
    both(gc, "wait", 0)
    both(gc, "start", 1)
    rs_step(7)
    d_second()
    both(gj, "start", 0)
    gq.finish()
    both(gc, "wait", 1)
    cross = jnp.sum(CR[...].astype(F32).reshape(16, 16, 512), axis=0).astype(BF16)
    term = jnp.dot(cross, QT[...].reshape(512, 1024), preferred_element_type=F32)
    recv(RRP.at[7], rpr.at[7])
    recv(RRM.at[6], rmr.at[6])
    total = WOWN[z] + RRP[7].astype(F32) + RRM[6].astype(F32)
    WT[16 * k + z] = (total + term).astype(BF16)
    gw.start()
    both(gj, "wait", 0)
    both(gj, "start", 1)
    gw.step(0)
    gw.step(1)
    gw.step(2)
    both(gj, "wait", 1)
    gw.step(3)
    loads[6].wait()

    def tiles(dst, base, left, right):
        @pl.loop(0, 4)
        def _(j):
            at = pl.ds(pl.multiple_of(j * HALF, HALF), HALF)
            weights = right[:, :, at].reshape(512, HALF)
            part = jnp.dot(left, weights, preferred_element_type=F32)
            dst[:, at] = (base[:, at].astype(F32) + part).astype(dst.dtype)

    tiles(ACC, C, PJ[...].reshape(512, 512), QT)
    for s in range(4, 8):
        gw.step(s)
    gw.finish()
    tiles(OUT, ACC, U[...], WT)
    store = pltpu.make_async_copy(OUT, out_h, load_sem.at[7])
    store.start()
    for copy in pending:
        copy.wait_send()

    @pl.when(diag)
    def _():
        n = 0
        for d in (8, 7, 9, 6, 10, 5, 11, 4, 12, 3, 13, 2, 14, 1, 15):
            for kk in (0, 1):
                cross_copy(d, kk, n).wait_send()
                n += 1
        pltpu.make_async_remote_copy(
            src_ref=CS.at[1 - k, z], dst_ref=CIN.at[k], send_sem=csnd.at[n], recv_sem=cinsem.at[k],
            device_id=sib, device_id_type=MESH,
        ).wait_send()

    store.wait()


def per_device(a, b, c, u, v, p, q):
    dma = pltpu.SemaphoreType.DMA
    anywhere = pl.BlockSpec(memory_space=pl.ANY)
    vm = pltpu.VMEM
    scratch = [
        vm((32, 16, 1024), BF16),
        vm((32, 16, 1024), BF16),
        vm((4, 4, 32, 512), BF16),
        vm((4, 4, 32, 512), BF16),
        vm((512, 512), BF16),
        vm((512, 1024), BF16),
        vm((512, 1024), BF16),
        vm((512, 1024), BF16),
        vm((512, 1024), BF16),
        vm((16, 16, 1024), F32),
        vm((16, 16, 1024), F32),
        vm((16, 16, 1024), F32),
        vm((8, 16, 1024), BF16),
        vm((8, 16, 1024), BF16),
        vm((7, 16, 1024), BF16),
        vm((7, 16, 1024), BF16),
        vm((32, 16, 1024), BF16),
        vm((2, 16, 16, 512), BF16),
        vm((2, 16, 512), BF16),
        vm((4, 4, 16, 512), BF16),
        vm((4, 4, 32, 512), F32),
        vm((4, 4, 32, 512), BF16),
        vm((2, 3, 4, 32, HALF), BF16),
        vm((2, 4, 32, HALF), F32),
        vm((2, 4, 32, HALF), BF16),
        vm((2, 3, 32, HALF), BF16),
        vm((4, 4, 32, 512), BF16),
        vm((512, 1024), F32),
        dma((8,)),
        dma((32,)), dma((31,)),
        dma((32,)), dma((31,)),
        dma((32,)), dma((31,)),
        dma, dma,
        dma((8,)), dma((8,)),
        dma((7,)), dma((7,)),
        dma((12,)), dma((12,)),
        dma((12,)), dma((12,)),
        dma((12,)), dma((12,)),
        dma((12,)), dma((12,)),
        dma((12,)), dma((12,)),
        dma((2,)), dma((31,)),
    ]
    return pl.pallas_call(
        kernel,
        out_shape=jax.ShapeDtypeStruct(c.shape, c.dtype),
        in_specs=[anywhere] * 7,
        out_specs=anywhere,
        scratch_shapes=scratch,
        compiler_params=pltpu.CompilerParams(
            collective_id=0, has_side_effects=True, vmem_limit_bytes=48 * 1024 * 1024
        ),
        name="maintain",
    )(v.T, u.T, p.T, q.T, a, b, c)


def solution(mesh):
    split = Mesh(mesh.devices.reshape(NZ, 2, 4, 4), ("z", "k", "x", "y"))
    row, col = ("z", "k"), ("x", "y")
    placed = (
        P(row, col), P(row, col), P(row, col), P(row, col), P(row, col), P(col, row), P(col, row),
    )
    return jax.shard_map(
        per_device, mesh=split, in_specs=placed, out_specs=P(row, col), check_vma=False
    )
```

```python
import jax
import jax.numpy as jnp
from jax import lax
from jax.experimental import pallas as pl
from jax.experimental.pallas import tpu as pltpu
from jax.sharding import Mesh
from jax.sharding import PartitionSpec as P

MESH = pl.DeviceIdType.MESH
F32 = jnp.float32
BF16 = jnp.bfloat16
NZ = 16
HALF = 256
NT = (((1,), (1,)), ((), ()))
STEPS = (1, 3, 2)


def rem(a, n):
    return lax.rem(a + 2 * n, n)


def kernel(
    vt_h, ut_h, pt_h, qt_h, a_h, b_h, c_h, OUT,
    PT, QT, VT, VS, UU, UN, U, A, AX, B, BX, C, W,
    RSP, RRP, RSM, RRM, LSP, LRP, LSM, LRM, WT,
    XV, CR, DF, DS, R1, EF, ES, R2, PJ, PN, ACC,
    load_sem, xrcv, xsnd, psem, psnd, pfwd, qsem, qsnd, qfwd, wsem, wsnd, wfwd, phalf,
    rpr, rmr, lpr, lmr, rsnd, vsem, vsnd, usem, usnd, crsem, crsnd,
    dsem, dsnd, jsem, jsnd, scsem, scsnd, scfar, free, known, told,
):
    z = lax.axis_index("z")
    k = lax.axis_index("k")
    x = lax.axis_index("x")
    y = lax.axis_index("y")
    sib = {"k": 1 - k}
    zp, zm = {"z": rem(z + 1, NZ)}, {"z": rem(z - 1, NZ)}
    zpp, zmm = {"z": rem(z + 2, NZ)}, {"z": rem(z - 2, NZ)}
    pos = {"x": x, "y": y}
    diag = z == 4 * x + y

    def send(src, dst, ssem, rsem, dev):
        pltpu.make_async_remote_copy(
            src_ref=src, dst_ref=dst, send_sem=ssem, recv_sem=rsem,
            device_id=dev, device_id_type=MESH,
        ).start()

    def recv(dst, rsem):
        pltpu.make_async_remote_copy(
            src_ref=dst, dst_ref=dst, send_sem=rsem, recv_sem=rsem,
            device_id=sib, device_id_type=MESH,
        ).wait_recv()

    def sent(ref, ssem):
        pltpu.make_async_remote_copy(
            src_ref=ref, dst_ref=ref, send_sem=ssem, recv_sem=ssem,
            device_id=sib, device_id_type=MESH,
        ).wait_send()

    low, high = pl.ds(0, 512), pl.ds(512, 512)
    own_lanes = pl.ds(pl.multiple_of(512 * k, 512), 512)
    loads = [
        pltpu.make_async_copy(pt_h, PT.at[z, k], load_sem.at[0]),
        pltpu.make_async_copy(vt_h, VT.at[x, y, :, own_lanes], load_sem.at[1]),
        pltpu.make_async_copy(qt_h, QT.at[z, k], load_sem.at[2]),
        pltpu.make_async_copy(ut_h, UU.at[x, y, k], load_sem.at[3]),
        pltpu.make_async_copy(b_h, B, load_sem.at[4]),
        pltpu.make_async_copy(a_h, A, load_sem.at[5]),
        pltpu.make_async_copy(c_h, C, load_sem.at[6]),
    ]
    for copy in loads:
        copy.start()

    barrier = pltpu.get_barrier_semaphore()
    near = [zp, zm, zpp, zmm]
    for axis in ("x", "y"):
        for step in STEPS:
            near.append({axis: rem(pos[axis] + step, 4)})
    peers = [sib] + [{**dev, "k": kk} for dev in near for kk in (0, 1)]
    for dev in peers:
        pl.semaphore_signal(barrier, inc=1, device_id=dev, device_id_type=MESH)
    pl.semaphore_wait(barrier, len(peers))

    class ZWide:
        def __init__(self, buf, rsem, ssem, fwd, part=slice(None)):
            self.buf, self.rsem, self.ssem, self.fwd, self.part = buf, rsem, ssem, fwd, part

        def at(self, d):
            return self.buf.at[rem(z - d, NZ), self.part]

        def place(self, d):
            return d - 1 if d > 0 else 7 - d

        def out(self, ref, d):
            dev = {1: zp, 2: zpp, -1: zm, -2: zmm}[d if abs(d) < 3 else (2 - d % 2) * (1 if d > 0 else -1)]
            send(ref, ref, self.ssem, self.rsem.at[self.place(d)], dev)

        def arrive(self, d):
            ref = self.at(d)
            recv(ref, self.rsem.at[self.place(d)])
            return ref

        def share(self, d):
            ref = self.at(d)
            send(ref, ref, self.ssem, self.fwd.at[0 if abs(d) < 6 else 1], sib)

        def own(self):
            return self.at(0)

        def start(self):
            self.out(self.own(), 2)
            self.out(self.own(), -2)

        def leaves(self, j):
            for sign in (1, -1):
                self.out(self.at(2 * j * sign) if j else self.own(), (2 * j + 1) * sign)

        def hub(self, j):
            self.on(j)
            self.off(j)

        def on(self, j):
            for sign, most in ((1, 8), (-1, 7)):
                d = 2 * j * sign
                ref = self.arrive(d)
                if 2 * j + 2 <= most:
                    self.out(ref, d + 2 * sign)

        def off(self, j):
            self.leaves(j - 1)
            if j == 3:
                self.leaves(3)
            self.share(2 * j)
            self.share(-2 * j)

        def leaf(self, j):
            for sign in (1, -1):
                d = (2 * j + 1) * sign
                self.arrive(d)
                self.share(d)

        def last(self):
            self.arrive(8)
            self.share(8)

        def shared(self, group):
            recv(self.buf.at[pl.ds(0, 5 if group else 10), self.part], self.fwd.at[group])

        def done(self):
            sent(self.buf.at[pl.ds(0, 15)], self.ssem)

    class ZNear(ZWide):
        def out(self, ref, d):
            send(ref, ref, self.ssem, self.rsem.at[self.place(d)], zp if d > 0 else zm)

        def start(self):
            self.leaves(0)

        def step(self, s):
            for sign, most in ((1, 8), (-1, 7)):
                if s < most:
                    d = sign * (s + 1)
                    ref = self.arrive(d)
                    if s + 1 < most:
                        self.out(ref, d + sign)
                    self.share(d)

    class ZHalves(ZWide):
        def own(self):
            return self.buf.at[z, k]

        def out(self, ref, d):
            if abs(d) > 2:
                super().out(ref, d)
                return
            dev = {1: zp, 2: zpp, -1: zm, -2: zmm}[d]
            place = 4 * k + {1: 0, 2: 1, -1: 2, -2: 3}[d]
            send(ref, ref, self.ssem, phalf.at[place], {**dev, "k": 1})

        def arrive(self, d):
            if abs(d) > 2:
                return super().arrive(d)
            for kk in (0, 1):
                recv(self.buf.at[rem(z - d, NZ), kk], phalf.at[4 * kk + {1: 0, 2: 1, -1: 2, -2: 3}[d]])
            return self.at(d)

        def done(self):
            sent(W.at[pl.ds(0, 14)], self.ssem)

    class PlaneGather:
        def __init__(self, buf, lanes, first, rsem, ssem, base, to):
            self.buf, self.lanes, self.first = buf, lanes, first
            self.rsem, self.ssem, self.base = rsem, ssem, base
            self.mid = (slice(None),) * (len(buf.shape) - 3)
            self.to = to

        def view(self, phase, at):
            if phase == 0:
                spot = {**pos, self.first: at}
                return self.buf.at[(spot["x"], spot["y"], *self.mid, self.lanes)]
            if self.first == "x":
                return self.buf.at[(slice(None), at, *self.mid, self.lanes)]
            return self.buf.at[(at, slice(None), *self.mid, self.lanes)]

        def axis(self, phase):
            return self.first if phase == 0 else ("y" if self.first == "x" else "x")

        def start(self, phase):
            axis = self.axis(phase)
            mine = self.view(phase, pos[axis])
            for step in STEPS:
                dev = {axis: rem(pos[axis] + step, 4), **self.to}
                send(mine, mine, self.ssem.at[phase], self.rsem.at[self.base + phase], dev)

        def wait(self, phase):
            some = (pl.ds(0, 3), slice(None)) if phase else (0, pl.ds(0, 3))
            recv(self.buf.at[(*some, *self.mid, self.lanes)], self.rsem.at[self.base + phase])

    lanes = [pl.ds(0, HALF), pl.ds(HALF, HALF)]
    order = ["x", "y"]

    def halves(buf, rsem, ssem, cut=lanes, to={}):
        return [PlaneGather(buf, cut[h], order[h], rsem, ssem, 2 * h, to) for h in (0, 1)]

    def plane_done(buf, ssem):
        sent(buf.at[0, pl.ds(0, 3)], ssem.at[0])
        sent(buf.at[pl.ds(0, 3)], ssem.at[1])

    gp = ZHalves(PT, psem, psnd, pfwd)
    gw = [ZWide(WT, wsem.at[i], wsnd.at[i], wfwd.at[i], i) for i in (0, 1)]
    gq = [ZNear(QT, qsem.at[i], qsnd.at[i], qfwd.at[i], i) for i in (0, 1)]
    gv = halves(VT, vsem, vsnd, [low, high], {"k": 1})
    gu = halves(UU, usem, usnd)
    gc = halves(CR, crsem, crsnd)
    gj = halves(PJ, jsem, jsnd)

    def both(gathers, what, phase):
        for g in gathers:
            getattr(g, what)(phase)

    def tiles(dst, base, left, right):
        for j in range(4):
            at = pl.ds(j * HALF, HALF)
            weights = right[..., at].reshape(512, HALF)
            part = jnp.dot(left, weights, preferred_element_type=F32)
            dst[:, at] = (base[:, at].astype(F32) + part).astype(dst.dtype)

    def rs_out(d, parts, src, dst, rsem, i, dev):
        total = W[d]
        for ref, sem, n in parts:
            recv(ref.at[n], sem.at[n])
            total = total + ref[n].astype(F32)
        src[i] = total.astype(BF16)
        send(src.at[i], dst.at[i], rsnd, rsem.at[i], dev)

    def rs_plus(i):
        parts = [(LRP, lpr, i - 1), (RRP, rpr, i - 1)] if i else []
        rs_out(rem(z + 8 - 2 * i, NZ), parts, RSP, RRP, rpr, i, zpp)

    def rs_minus(i):
        parts = [(LRM, lmr, i)] + ([(RRM, rmr, i - 1)] if i else [])
        rs_out(rem(z - 6 + 2 * i, NZ), parts, RSM, RRM, rmr, i, zmm)

    def rs_leaf(i):
        rs_out(rem(z - 7 + 2 * i, NZ), [], LSM, LRM, lmr, i, zm)
        rs_out(rem(z + 7 - 2 * i, NZ), [], LSP, LRP, lpr, i, zp)

    def sum_w():
        left = VT[...].reshape(512, 1024)
        for j in range(4):
            at = pl.ds(j * HALF, HALF)
            part = jnp.dot(left[:, :512], BX[:, at], preferred_element_type=F32)
            part = part + jnp.dot(left[:, 512:], B[:, at], preferred_element_type=F32)
            W[:, :, at] = part.reshape(NZ, 32, HALF)

    def cross_part():
        part = lax.dot_general(XV[...], PT[...].reshape(512, 1024), NT, preferred_element_type=F32)
        CR[x, y] = part.astype(BF16)

    def own_w():
        cross = jnp.sum(CR[...].astype(F32).reshape(16, 32, 512), axis=0).astype(BF16)
        total = W[z] + jnp.dot(cross, QT[...].reshape(512, 1024), preferred_element_type=F32)
        for ref, sem, n in ((LRP, lpr, 3), (LRM, lmr, 3), (RRP, rpr, 3), (RRM, rmr, 2)):
            recv(ref.at[n], sem.at[n])
            total = total + ref[n].astype(F32)
        WT[z] = total.astype(BF16).reshape(2, 16, 1024)

    def w_start():
        for g in gw:
            g.start()

    def w_hub(j):
        for g in gw:
            g.on(j)
        for g in gw:
            g.off(j)

    def w_leaf(j):
        for g in gw:
            g.leaf(j)

    def w_last():
        for g in gw:
            g.last()

    def q_step(s):
        for g in gq:
            g.step(s)

    def tell(i):
        pl.semaphore_signal(told.at[i], inc=1, device_id=zpp, device_id_type=MESH)
        pl.semaphore_signal(told.at[3 + i], inc=1, device_id=zmm, device_id_type=MESH)

    def hear(i):
        pl.semaphore_wait(told.at[i], 1)
        pl.semaphore_wait(told.at[3 + i], 1)

    far = (8, 7, 9, 6, 10, 5, 11)
    close = (4, 12, 3, 13, 2, 14, 1, 15, 0)

    def scatter_some(some, src, ssem):
        for d in some:
            zz = rem(z + d, NZ)
            send(src.at[zz // 4, lax.rem(zz, 4)], XV, ssem, scsem, {"z": zz, "k": 1})

    def pass_v():
        return pltpu.make_async_remote_copy(
            src_ref=VT, dst_ref=VS, send_sem=xsnd.at[3], recv_sem=xrcv.at[3],
            device_id=sib, device_id_type=MESH,
        )

    @pl.when(k == 1)
    def _():
        loads[1].wait()
        gv[1].start(0)
        loads[0].wait()
        gp.start()
        loads[2].wait()
        send(QT.at[z, 1], QT.at[z, 1], xsnd.at[0], xrcv.at[0], sib)
        loads[3].wait()
        send(UU.at[x, y, 1], UU.at[x, y, 1], xsnd.at[1], xrcv.at[1], sib)
        send(PT.at[z, 1], PT.at[z, 1], xsnd.at[5], xrcv.at[5], sib)
        send(a_h, AX, xsnd.at[2], xrcv.at[2], sib)
        gv[1].wait(0)
        gv[1].start(1)
        recv(VT.at[x, y, :, low], xrcv.at[1])
        gv[0].wait(0)
        gv[0].start(1)
        gp.hub(1)
        gp.hub(2)
        gp.leaf(0)
        gv[1].wait(1)
        gv[0].wait(1)

        pl.semaphore_wait(known, 1)

        @pl.when(diag)
        def _():
            pass_v().start()
            scatter_some(far, VT, scfar)

        loads[4].wait()
        recv(BX, xrcv.at[2])
        sum_w()
        rs_plus(0)
        rs_leaf(0)
        gp.hub(3)
        gp.leaf(1)
        gp.leaf(2)
        rs_minus(0)
        rs_leaf(1)
        gp.last()
        gp.leaf(3)
        rs_plus(1)
        rs_minus(1)
        rs_leaf(2)
        recv(PT.at[z, 0], xrcv.at[0])
        recv(XV, scsem)
        cross_part()
        both(gc, "start", 0)
        rs_plus(2)
        rs_minus(2)
        rs_leaf(3)
        both(gc, "wait", 0)
        both(gc, "start", 1)
        rs_plus(3)
        recv(QT.at[z, 0], xrcv.at[5])
        for g in gq:
            g.shared(0)
            g.shared(1)
        both(gc, "wait", 1)
        pl.semaphore_signal(free, inc=1, device_id=sib, device_id_type=MESH)
        own_w()
        w_start()
        send(WT.at[z], WT.at[z], xsnd.at[4], xrcv.at[4], sib)
        w_hub(1)
        w_hub(2)
        w_leaf(0)
        loads[6].wait()
        loads[5].wait()
        recv(UN, xrcv.at[4])
        U[...] = UN[...].reshape(512, 512).T
        w_hub(3)
        w_leaf(1)
        for h in (0, 1):
            recv(PN.at[:, :, :, lanes[h]], xrcv.at[6 + h])
        tiles(ACC, C, PN[...].reshape(512, 512), QT)
        w_leaf(2)
        w_last()
        w_leaf(3)
        tiles(OUT, ACC, U[...], WT)
        gp.done()
        for g in gw:
            g.done()
        sent(PT.at[pl.ds(0, 15)], rsnd)
        sent(VT.at[0, pl.ds(0, 3), :, low], vsnd.at[0])
        sent(VT.at[pl.ds(0, 3)], vsnd.at[1])
        plane_done(CR, crsnd)
        sent(QT.at[z, 1], xsnd.at[0])
        sent(UU.at[x, y, 1], xsnd.at[1])
        sent(AX, xsnd.at[2])
        sent(WT.at[z], xsnd.at[4])
        sent(PT.at[z, 1], xsnd.at[5])

        @pl.when(diag)
        def _():
            pass_v().wait_send()
            sent(PT.at[pl.ds(0, 7)], scfar)


    def d_part(h):
        points = PT[pl.ds(8 * h, 8)].reshape(HALF, 1024)
        for r, left in ((0, A), (1, AX)):
            part = lax.dot_general(left[...], points, NT, preferred_element_type=F32).reshape(4, 4, 32, HALF)
            DF[:, :, r, :, lanes[h]] = part
            DS[:, :, r, :, lanes[h]] = part.astype(BF16)

    def d_start(h, phase):
        axis = order[h] if phase == 0 else order[1 - h]
        for i, step in enumerate(STEPS):
            t = rem(pos[axis] + step, 4)
            if phase == 1:
                src, dst = ES.at[h, t], R2.at[h, i]
            else:
                src = DS.at[t, :, :, :, lanes[h]] if h == 0 else DS.at[:, t, :, :, lanes[h]]
                dst = R1.at[h, i]
            send(src, dst, dsnd.at[phase], dsem.at[2 * h + phase], {axis: t})

    def d_first(h):
        recv(R1.at[h], dsem.at[2 * h])
        total = DF[x, :, :, :, lanes[h]] if h == 0 else DF[:, y, :, :, lanes[h]]
        for i in range(3):
            total = total + R1[h, i].astype(F32)
        EF[h] = total
        ES[h] = total.astype(BF16)
        d_start(h, 1)

    def d_second(h):
        recv(R2.at[h], dsem.at[2 * h + 1])
        total = EF[h, pos[order[1 - h]]]
        for i in range(3):
            total = total + R2[h, i].astype(F32)
        PJ[x, y, :, :, lanes[h]] = total.astype(BF16)

    @pl.when(k == 0)
    def _():
        tell(0)
        loads[1].wait()
        gv[0].start(0)
        loads[0].wait()
        gp.start()
        send(VT.at[x, y, :, low], VT.at[x, y, :, low], xsnd.at[1], xrcv.at[1], sib)
        loads[2].wait()
        gq[0].start()
        recv(QT.at[z, 1], xrcv.at[0])
        gq[1].start()
        gp.leaves(0)
        send(b_h, BX, xsnd.at[2], xrcv.at[2], sib)
        send(PT.at[z, 0], PT.at[z, 0], xsnd.at[0], xrcv.at[0], sib)
        send(QT.at[z, 0], QT.at[z, 0], xsnd.at[5], xrcv.at[5], sib)
        loads[3].wait()
        recv(UU.at[x, y, 1], xrcv.at[1])
        hear(0)
        tell(1)
        q_step(0)
        hear(1)
        tell(2)
        q_step(1)
        hear(2)
        pl.semaphore_signal(known, inc=1, device_id=sib, device_id_type=MESH)
        q_step(2)
        both(gu, "start", 0)
        q_step(3)

        @pl.when(diag)
        def _():
            recv(VS, xrcv.at[3])
            scatter_some(close, VS, scsnd)

        q_step(4)

        both(gu, "wait", 0)
        both(gu, "start", 1)
        recv(PT.at[z, 1], xrcv.at[5])
        gp.shared(0)
        q_step(5)

        loads[5].wait()
        recv(AX, xrcv.at[2])
        gp.shared(1)
        d_part(0)
        d_start(0, 0)
        d_part(1)
        d_start(1, 0)
        q_step(6)
        d_first(0)
        d_first(1)
        q_step(7)
        both(gu, "wait", 1)
        send(UU.at[:, :, 1], UN, xsnd.at[4], xrcv.at[4], sib)
        U[...] = UU[:, :, 0].reshape(512, 512).T
        d_second(0)
        d_second(1)
        pl.semaphore_wait(free, 1)
        both(gj, "start", 0)
        for g in gj:
            g.wait(0)
            g.start(1)
        loads[6].wait()
        loads[4].wait()
        for h in (0, 1):
            gj[h].wait(1)
            send(PJ.at[:, :, 1, :, lanes[h]], PN.at[:, :, :, lanes[h]], xsnd.at[6 + h], xrcv.at[6 + h], sib)
        tiles(ACC, C, PJ[:, :, 0].reshape(512, 512), QT)
        recv(WT.at[z], xrcv.at[4])
        for g in gw:
            g.shared(0)
        for g in gw:
            g.shared(1)
        tiles(OUT, ACC, U[...], WT)
        for g in gq:
            g.done()
        sent(PT.at[pl.ds(0, 2)], psnd)
        sent(VT.at[0, pl.ds(0, 3), :, low], vsnd.at[0])
        plane_done(UU, usnd)
        plane_done(PJ, jsnd)
        sent(R1, dsnd.at[0])
        sent(R2, dsnd.at[1])
        sent(PT.at[z, 0], xsnd.at[0])
        sent(VT.at[x, y, :, low], xsnd.at[1])
        sent(BX, xsnd.at[2])
        sent(QT.at[z, 0], xsnd.at[5])
        sent(UN, xsnd.at[4])
        for h in (0, 1):
            sent(PN.at[:, :, :, lanes[h]], xsnd.at[6 + h])

        @pl.when(diag)
        def _():
            sent(PT.at[pl.ds(0, 9)], scsnd)


def per_device(a, b, c, u, v, p, q):
    dma = pltpu.SemaphoreType.DMA
    anywhere = pl.BlockSpec(memory_space=pltpu.HBM)
    vm = pltpu.VMEM
    scratch = [
        vm((16, 2, 16, 1024), BF16),
        vm((16, 2, 16, 1024), BF16),
        vm((4, 4, 32, 1024), BF16),
        vm((4, 4, 32, 1024), BF16),
        vm((4, 4, 2, 32, 512), BF16),
        vm((4, 4, 32, 512), BF16),
        vm((512, 512), BF16),
        *[vm((512, 1024), BF16) for _ in range(5)],
        vm((16, 32, 1024), F32),
        *[vm((n, 32, 1024), BF16) for n in (4, 4, 3, 3, 4, 4, 4, 4)],
        vm((16, 2, 16, 1024), BF16),
        vm((32, 1024), BF16),
        vm((4, 4, 32, 512), BF16),
        vm((4, 4, 2, 32, 512), F32),
        vm((4, 4, 2, 32, 512), BF16),
        vm((2, 3, 4, 2, 32, HALF), BF16),
        vm((2, 4, 2, 32, HALF), F32),
        vm((2, 4, 2, 32, HALF), BF16),
        vm((2, 3, 2, 32, HALF), BF16),
        vm((4, 4, 2, 32, 512), BF16),
        vm((4, 4, 32, 512), BF16),
        vm((512, 1024), F32),
        dma((7,)), dma((8,)), dma((8,)),
        dma((15,)), dma, dma((2,)),
        *[dma((2, 15)), dma((2,)), dma((2, 2))] * 2,
        dma((8,)),
        dma((4,)), dma((3,)), dma((4,)), dma((4,)), dma,
        *[dma((4,)), dma((2,))] * 5,
        dma, dma, dma, pltpu.SemaphoreType.REGULAR, pltpu.SemaphoreType.REGULAR, pltpu.SemaphoreType.REGULAR((6,)),
    ]
    return pl.pallas_call(
        kernel,
        out_shape=jax.ShapeDtypeStruct(c.shape, c.dtype),
        in_specs=[anywhere] * 7,
        out_specs=pl.BlockSpec(memory_space=pltpu.VMEM),
        scratch_shapes=scratch,
        compiler_params=pltpu.CompilerParams(
            collective_id=0, has_side_effects=True, vmem_limit_bytes=67043328
        ),
        name="maintain",
    )(v.T, u.T, p.T, q.T, a, b, c)


def solution(mesh):
    split = Mesh(mesh.devices.reshape(NZ, 2, 4, 4), ("z", "k", "x", "y"))
    row, col = ("z", "k"), ("x", "y")
    placed = (
        P(row, col), P(row, col), P(row, col), P(row, col), P(row, col), P(col, row), P(col, row),
    )
    return jax.shard_map(
        per_device, mesh=split, in_specs=placed, out_specs=P(row, col), check_vma=False
    )
```

```python
import jax
import jax.numpy as jnp
from jax import lax
from jax.experimental import pallas as pl
from jax.experimental.pallas import tpu as pltpu
from jax.sharding import Mesh
from jax.sharding import PartitionSpec as P

MESH = pl.DeviceIdType.MESH
F32 = jnp.float32
BF16 = jnp.bfloat16
NZ = 16
HALF = 256
NT = (((1,), (1,)), ((), ()))
STEPS = (1, 3, 2)


def rem(a, n):
    return lax.rem(a + 2 * n, n)


def kernel(
    vt_h, ut_h, pt_h, qt_h, a_h, b_h, c_h, out_h,
    PT, QT, VT, UU, UN, U, A, AX, B, BX, C, W,
    RSP, RRP, RSM, RRM, LSP, LRP, LSM, LRM, WT,
    OUT, XV, TV, CR, DF, DS, R1, EF, ES, R2, PJ, PN, ACC,
    load_sem, xrcv, xsnd, psem, psnd, pfwd, qsem, qsnd, qfwd, wsem, wsnd, wfwd,
    rpr, rmr, lpr, lmr, rsnd, vsem, vsnd, usem, usnd, crsem, crsnd,
    dsem, dsnd, jsem, jsnd, scsem, scsnd, tvsem, tusnd, free, known, told,
):
    z = lax.axis_index("z")
    k = lax.axis_index("k")
    x = lax.axis_index("x")
    y = lax.axis_index("y")
    sib = {"k": 1 - k}
    zp, zm = {"z": rem(z + 1, NZ)}, {"z": rem(z - 1, NZ)}
    zpp, zmm = {"z": rem(z + 2, NZ)}, {"z": rem(z - 2, NZ)}
    pos = {"x": x, "y": y}
    c = 4 * x + y
    gap = rem(c - z, NZ)
    even = lax.rem(gap, 2) == 0

    def send(src, dst, ssem, rsem, dev):
        pltpu.make_async_remote_copy(
            src_ref=src, dst_ref=dst, send_sem=ssem, recv_sem=rsem,
            device_id=dev, device_id_type=MESH,
        ).start()

    def recv(dst, rsem):
        pltpu.make_async_remote_copy(
            src_ref=dst, dst_ref=dst, send_sem=rsem, recv_sem=rsem,
            device_id=sib, device_id_type=MESH,
        ).wait_recv()

    def sent(ref, ssem):
        pltpu.make_async_remote_copy(
            src_ref=ref, dst_ref=ref, send_sem=ssem, recv_sem=ssem,
            device_id=sib, device_id_type=MESH,
        ).wait_send()

    low, high = pl.ds(0, 512), pl.ds(512, 512)
    own_lanes = pl.ds(pl.multiple_of(512 * k, 512), 512)
    loads = [
        pltpu.make_async_copy(pt_h, PT.at[z, k], load_sem.at[0]),
        pltpu.make_async_copy(vt_h, VT.at[x, y, :, own_lanes], load_sem.at[1]),
        pltpu.make_async_copy(qt_h, QT.at[z, k], load_sem.at[2]),
        pltpu.make_async_copy(ut_h, UU.at[x, y, k], load_sem.at[3]),
        pltpu.make_async_copy(b_h, B, load_sem.at[4]),
        pltpu.make_async_copy(a_h, A, load_sem.at[5]),
        pltpu.make_async_copy(c_h, C, load_sem.at[6]),
    ]
    for copy in loads:
        copy.start()

    barrier = pltpu.get_barrier_semaphore()
    near = [zp, zm, zpp, zmm]
    for axis in ("x", "y"):
        for step in STEPS:
            near.append({axis: rem(pos[axis] + step, 4)})
    peers = [sib] + [{**dev, "k": kk} for dev in near for kk in (0, 1)]
    for dev in peers:
        pl.semaphore_signal(barrier, inc=1, device_id=dev, device_id_type=MESH)
    pl.semaphore_wait(barrier, len(peers))

    class ZWide:
        def __init__(self, buf, rsem, ssem, fwd, part, to={}):
            self.buf, self.rsem, self.ssem, self.fwd, self.part, self.to = buf, rsem, ssem, fwd, part, to

        def at(self, d):
            return self.buf.at[rem(z - d, NZ), self.part]

        def place(self, d):
            return d - 1 if d > 0 else 7 - d

        def out(self, ref, d):
            dev = {1: zp, 2: zpp, -1: zm, -2: zmm}[d if abs(d) < 3 else (2 - d % 2) * (1 if d > 0 else -1)]
            send(ref, ref, self.ssem, self.rsem.at[self.place(d)], {**dev, **self.to})

        def arrive(self, d):
            ref = self.at(d)
            recv(ref, self.rsem.at[self.place(d)])
            return ref

        def share(self, d):
            ref = self.at(d)
            send(ref, ref, self.ssem, self.fwd.at[0 if abs(d) < 6 else 1], sib)

        def start(self):
            self.out(self.at(0), 2)
            self.out(self.at(0), -2)

        def leaves(self, j):
            for sign in (1, -1):
                self.out(self.at(2 * j * sign), (2 * j + 1) * sign)

        def on(self, j):
            for sign, most in ((1, 8), (-1, 7)):
                d = 2 * j * sign
                ref = self.arrive(d)
                if 2 * j + 2 <= most:
                    self.out(ref, d + 2 * sign)

        def off(self, j, skip=False):
            if not skip:
                self.leaves(j - 1)
            if j == 3:
                self.leaves(3)
            self.share(2 * j)
            self.share(-2 * j)

        def leaf(self, j):
            for sign in (1, -1):
                d = (2 * j + 1) * sign
                self.arrive(d)
                self.share(d)

        def last(self):
            self.arrive(8)
            self.share(8)

        def shared(self, group):
            recv(self.buf.at[pl.ds(0, 5 if group else 10), self.part], self.fwd.at[group])

        def done(self):
            sent(self.buf.at[pl.ds(0, 15)], self.ssem)

    class ZNear(ZWide):
        def out(self, ref, d):
            send(ref, ref, self.ssem, self.rsem.at[self.place(d)], zp if d > 0 else zm)

        def start(self):
            self.leaves(0)

        def step(self, s):
            for sign, most in ((1, 8), (-1, 7)):
                if s < most:
                    d = sign * (s + 1)
                    ref = self.arrive(d)
                    if s + 1 < most:
                        self.out(ref, d + sign)
                    self.share(d)

    class PlaneGather:
        def __init__(self, buf, lanes, first, rsem, ssem, base, to):
            self.buf, self.lanes, self.first = buf, lanes, first
            self.rsem, self.ssem, self.base = rsem, ssem, base
            self.mid = (slice(None),) * (len(buf.shape) - 3)
            self.to = to

        def view(self, phase, at):
            if phase == 0:
                spot = {**pos, self.first: at}
                return self.buf.at[(spot["x"], spot["y"], *self.mid, self.lanes)]
            if self.first == "x":
                return self.buf.at[(slice(None), at, *self.mid, self.lanes)]
            return self.buf.at[(at, slice(None), *self.mid, self.lanes)]

        def axis(self, phase):
            return self.first if phase == 0 else ("y" if self.first == "x" else "x")

        def start(self, phase):
            axis = self.axis(phase)
            mine = self.view(phase, pos[axis])
            for step in STEPS:
                dev = {axis: rem(pos[axis] + step, 4), **self.to}
                send(mine, mine, self.ssem.at[phase], self.rsem.at[self.base + phase], dev)

        def wait(self, phase):
            some = (pl.ds(0, 3), slice(None)) if phase else (0, pl.ds(0, 3))
            recv(self.buf.at[(*some, *self.mid, self.lanes)], self.rsem.at[self.base + phase])

    lanes = [pl.ds(0, HALF), pl.ds(HALF, HALF)]
    order = ["x", "y"]

    def halves(buf, rsem, ssem, cut=lanes, to={}):
        return [PlaneGather(buf, cut[h], order[h], rsem, ssem, 2 * h, to) for h in (0, 1)]

    def plane_done(buf, ssem):
        sent(buf.at[0, pl.ds(0, 3)], ssem.at[0])
        sent(buf.at[pl.ds(0, 3)], ssem.at[1])

    gp = [ZWide(PT, psem.at[i], psnd.at[i], pfwd.at[i], i, {"k": 1}) for i in (0, 1)]
    gw = [ZWide(WT, wsem.at[i], wsnd.at[i], wfwd.at[i], i) for i in (0, 1)]
    gq = [ZNear(QT, qsem.at[i], qsnd.at[i], qfwd.at[i], i) for i in (0, 1)]
    gv = halves(VT, vsem, vsnd, [low, high], {"k": 1})
    gu = halves(UU, usem, usnd)
    gc = halves(CR, crsem, crsnd)
    gj = halves(PJ, jsem, jsnd)

    def both(gathers, what, phase):
        for g in gathers:
            getattr(g, what)(phase)

    def tiles(dst, base, left, right):
        for j in range(4):
            at = pl.ds(j * HALF, HALF)
            weights = right[..., at].reshape(512, HALF)
            part = jnp.dot(left, weights, preferred_element_type=F32)
            dst[:, at] = (base[:, at].astype(F32) + part).astype(dst.dtype)
            if dst is OUT:
                result(j).start()

    def result(j):
        at = pl.ds(j * HALF, HALF)
        return pltpu.make_async_copy(OUT.at[:, at], out_h.at[:, at], load_sem.at[j])

    def stored():
        for j in range(4):
            result(j).wait()

    cols = [low, high]

    def rs_out(d, parts, src, dst, rsem, i, p, dev):
        total = W[d, :, cols[p]]
        for ref, sem, n in parts:
            recv(ref.at[n, :, cols[p]], sem.at[p, n])
            total = total + ref[n, :, cols[p]].astype(F32)
        src[i, :, cols[p]] = total.astype(BF16)
        send(src.at[i, :, cols[p]], dst.at[i, :, cols[p]], rsnd, rsem.at[p, i], dev)

    def rs_plus(i, p):
        parts = [(LRP, lpr, i - 1), (RRP, rpr, i - 1)] if i else []
        rs_out(rem(z + 8 - 2 * i, NZ), parts, RSP, RRP, rpr, i, p, zpp)

    def rs_minus(i, p):
        parts = [(LRM, lmr, i)] + ([(RRM, rmr, i - 1)] if i else [])
        rs_out(rem(z - 6 + 2 * i, NZ), parts, RSM, RRM, rmr, i, p, zmm)

    def rs_leaf(i, p):
        rs_out(rem(z - 7 + 2 * i, NZ), [], LSM, LRM, lmr, i, p, zm)
        rs_out(rem(z + 7 - 2 * i, NZ), [], LSP, LRP, lpr, i, p, zp)

    def rs_both(what, i):
        for p in (0, 1):
            what(i, p)

    def sum_w(p):
        left = VT[...].reshape(512, 1024)
        for j in (2 * p, 2 * p + 1):
            at = pl.ds(j * HALF, HALF)
            part = jnp.dot(left[:, :512], BX[:, at], preferred_element_type=F32)
            part = part + jnp.dot(left[:, 512:], B[:, at], preferred_element_type=F32)
            W[:, :, at] = part.reshape(NZ, 32, HALF)

    def cross_part():
        part = lax.dot_general(XV[...], PT[...].reshape(512, 1024), NT, preferred_element_type=F32)
        CR[x, y] = part.astype(BF16)

    def own_w():
        cross = jnp.sum(CR[...].astype(F32).reshape(16, 32, 512), axis=0).astype(BF16)
        total = W[z] + jnp.dot(cross, QT[...].reshape(512, 1024), preferred_element_type=F32)
        for ref, sem, n in ((LRP, lpr, 3), (LRM, lmr, 3), (RRP, rpr, 3), (RRM, rmr, 2)):
            for p in (0, 1):
                recv(ref.at[n, :, cols[p]], sem.at[p, n])
            total = total + ref[n].astype(F32)
        WT[z] = total.astype(BF16).reshape(2, 16, 1024)

    def p_hub(j):
        for g in gp:
            g.on(j)
        gp[0].off(j, j == 1)
        gp[1].off(j)

    def p_leaf(j):
        for g in gp:
            g.leaf(j)

    def w_start():
        for g in gw:
            g.start()

    def w_hub(j):
        for g in gw:
            g.on(j)
        for g in gw:
            g.off(j)

    def w_leaf(j):
        for g in gw:
            g.leaf(j)

    def w_last():
        for g in gw:
            g.last()

    def q_step(s):
        for g in gq:
            g.step(s)

    def tell(i):
        pl.semaphore_signal(told.at[i], inc=1, device_id=zpp, device_id_type=MESH)
        pl.semaphore_signal(told.at[3 + i], inc=1, device_id=zmm, device_id_type=MESH)

    def hear(i):
        pl.semaphore_wait(told.at[i], 1)
        pl.semaphore_wait(told.at[3 + i], 1)

    def scatter():
        def one(d):
            b = rem(z + d, NZ)
            send(VT.at[b // 4, lax.rem(b, 4)], TV, scsnd, tvsem, {"z": b, "k": 1})

        @pl.when(even & (gap != 0))
        def _():
            one(gap // 2)

        @pl.when(even)
        def _():
            one(gap // 2 + 8)

    def turn():
        @pl.when(gap != 0)
        def _():
            recv(TV, tvsem)

        @pl.when(lax.rem(gap, 8) != 0)
        def _():
            a = rem(2 * z - c, NZ)
            send(TV, XV, tusnd, scsem, {"k": 1, "x": a // 4, "y": lax.rem(a, 4)})

        @pl.when(gap == 8)
        def _():
            XV[...] = TV[...]

        @pl.when(gap == 0)
        def _():
            XV[...] = VT[x, y]

    def turned():
        @pl.when(lax.rem(gap, 8) != 0)
        def _():
            recv(XV, scsem)

    @pl.when(k == 1)
    def _():
        loads[1].wait()
        gv[1].start(0)
        loads[0].wait()
        gp[1].start()
        loads[2].wait()
        send(QT.at[z, 1], QT.at[z, 1], xsnd.at[0], xrcv.at[0], sib)
        loads[3].wait()
        send(UU.at[x, y, 1], UU.at[x, y, 1], xsnd.at[1], xrcv.at[1], sib)
        send(PT.at[z, 1], PT.at[z, 1], xsnd.at[5], xrcv.at[5], sib)
        send(a_h, AX, xsnd.at[2], xrcv.at[2], sib)
        gv[1].wait(0)
        gv[1].start(1)
        p_hub(1)
        recv(VT.at[x, y, :, low], xrcv.at[1])
        gv[0].wait(0)
        gv[0].start(1)
        p_hub(2)
        p_leaf(0)
        gv[1].wait(1)
        gv[0].wait(1)
        pl.semaphore_wait(known, 1)

        scatter()

        loads[4].wait()
        recv(BX, xrcv.at[2])
        for p in (0, 1):
            sum_w(p)
            rs_plus(0, p)
            rs_leaf(0, p)
        p_hub(3)
        p_leaf(1)
        rs_both(rs_minus, 0)
        rs_both(rs_leaf, 1)
        rs_both(rs_plus, 1)
        turn()
        rs_both(rs_minus, 1)
        rs_both(rs_leaf, 2)
        p_leaf(2)
        for g in gp:
            g.last()
        p_leaf(3)
        recv(PT.at[z, 0], xrcv.at[0])
        turned()
        cross_part()
        both(gc, "start", 0)
        rs_both(rs_plus, 2)
        both(gc, "wait", 0)
        both(gc, "start", 1)
        rs_both(rs_minus, 2)
        rs_both(rs_leaf, 3)
        rs_both(rs_plus, 3)
        recv(QT.at[z, 0], xrcv.at[5])
        for g in gq:
            g.shared(0)
            g.shared(1)
        both(gc, "wait", 1)
        pl.semaphore_signal(free, inc=1, device_id=sib, device_id_type=MESH)
        own_w()
        w_start()
        send(WT.at[z], WT.at[z], xsnd.at[4], xrcv.at[4], sib)
        w_hub(1)
        w_hub(2)
        w_leaf(0)
        loads[6].wait()
        loads[5].wait()
        recv(UN, xrcv.at[4])
        U[...] = UN[...].reshape(512, 512).T
        w_hub(3)
        w_leaf(1)
        for h in (0, 1):
            recv(PN.at[:, :, :, lanes[h]], xrcv.at[6 + h])
        tiles(ACC, C, PN[...].reshape(512, 512), QT)
        w_leaf(2)
        w_last()
        w_leaf(3)
        tiles(OUT, ACC, U[...], WT)
        sent(PT.at[pl.ds(0, 13)], psnd.at[0])
        for g in (gp[1], *gw):
            g.done()
        sent(PT.at[pl.ds(0, 15)], rsnd)
        sent(VT.at[0, pl.ds(0, 3), :, low], vsnd.at[0])
        sent(VT.at[pl.ds(0, 3)], vsnd.at[1])
        plane_done(CR, crsnd)
        sent(QT.at[z, 1], xsnd.at[0])
        sent(UU.at[x, y, 1], xsnd.at[1])
        sent(AX, xsnd.at[2])
        sent(WT.at[z], xsnd.at[4])
        sent(PT.at[z, 1], xsnd.at[5])

        @pl.when(even & (gap != 0))
        def _():
            sent(PT.at[pl.ds(0, 2)], scsnd)

        @pl.when(gap == 0)
        def _():
            sent(PT.at[0], scsnd)

        @pl.when(lax.rem(gap, 8) != 0)
        def _():
            sent(TV, tusnd)

        stored()


    def d_part(h):
        points = PT[pl.ds(8 * h, 8)].reshape(HALF, 1024)
        for r, left in ((0, A), (1, AX)):
            part = lax.dot_general(left[...], points, NT, preferred_element_type=F32).reshape(4, 4, 32, HALF)
            DF[:, :, r, :, lanes[h]] = part
            DS[:, :, r, :, lanes[h]] = part.astype(BF16)

    def d_start(h, phase):
        axis = order[h] if phase == 0 else order[1 - h]
        for i, step in enumerate(STEPS):
            t = rem(pos[axis] + step, 4)
            if phase == 1:
                src, dst = ES.at[h, t], R2.at[h, i]
            else:
                src = DS.at[t, :, :, :, lanes[h]] if h == 0 else DS.at[:, t, :, :, lanes[h]]
                dst = R1.at[h, i]
            send(src, dst, dsnd.at[phase], dsem.at[2 * h + phase], {axis: t})

    def d_first(h):
        recv(R1.at[h], dsem.at[2 * h])
        total = DF[x, :, :, :, lanes[h]] if h == 0 else DF[:, y, :, :, lanes[h]]
        for i in range(3):
            total = total + R1[h, i].astype(F32)
        EF[h] = total
        ES[h] = total.astype(BF16)
        d_start(h, 1)

    def d_second(h):
        recv(R2.at[h], dsem.at[2 * h + 1])
        total = EF[h, pos[order[1 - h]]]
        for i in range(3):
            total = total + R2[h, i].astype(F32)
        PJ[x, y, :, :, lanes[h]] = total.astype(BF16)

    @pl.when(k == 0)
    def _():
        tell(0)
        loads[1].wait()
        gv[0].start(0)
        loads[0].wait()
        gp[0].start()
        send(VT.at[x, y, :, low], VT.at[x, y, :, low], xsnd.at[1], xrcv.at[1], sib)
        loads[2].wait()
        gq[0].start()
        recv(QT.at[z, 1], xrcv.at[0])
        gq[1].start()
        gp[0].leaves(0)
        send(b_h, BX, xsnd.at[2], xrcv.at[2], sib)
        send(PT.at[z, 0], PT.at[z, 0], xsnd.at[0], xrcv.at[0], sib)
        send(QT.at[z, 0], QT.at[z, 0], xsnd.at[5], xrcv.at[5], sib)
        loads[3].wait()
        recv(UU.at[x, y, 1], xrcv.at[1])
        hear(0)
        tell(1)
        q_step(0)
        hear(1)
        tell(2)
        q_step(1)
        hear(2)
        pl.semaphore_signal(known, inc=1, device_id=sib, device_id_type=MESH)
        q_step(2)
        q_step(3)

        q_step(4)
        recv(PT.at[z, 1], xrcv.at[5])
        for g in gp:
            g.shared(0)
            g.shared(1)
        loads[5].wait()
        recv(AX, xrcv.at[2])
        d_part(0)
        d_start(0, 0)
        d_part(1)
        d_start(1, 0)
        both(gu, "start", 0)
        q_step(5)
        q_step(6)
        d_first(0)
        d_first(1)
        both(gu, "wait", 0)
        both(gu, "start", 1)
        q_step(7)
        d_second(0)
        d_second(1)
        pl.semaphore_wait(free, 1)
        both(gj, "start", 0)
        both(gu, "wait", 1)
        send(UU.at[:, :, 1], UN, xsnd.at[4], xrcv.at[4], sib)
        for g in gj:
            g.wait(0)
            g.start(1)
        U[...] = UU[:, :, 0].reshape(512, 512).T
        loads[6].wait()
        loads[4].wait()
        for h in (0, 1):
            gj[h].wait(1)
            send(PJ.at[:, :, 1, :, lanes[h]], PN.at[:, :, :, lanes[h]], xsnd.at[6 + h], xrcv.at[6 + h], sib)
        tiles(ACC, C, PJ[:, :, 0].reshape(512, 512), QT)
        recv(WT.at[z], xrcv.at[4])
        for g in gw:
            g.shared(0)
        for g in gw:
            g.shared(1)
        tiles(OUT, ACC, U[...], WT)
        for g in gq:
            g.done()
        sent(PT.at[pl.ds(0, 2)], psnd.at[0])
        sent(VT.at[0, pl.ds(0, 3), :, low], vsnd.at[0])
        plane_done(UU, usnd)
        plane_done(PJ, jsnd)
        sent(R1, dsnd.at[0])
        sent(R2, dsnd.at[1])
        sent(PT.at[z, 0], xsnd.at[0])
        sent(VT.at[x, y, :, low], xsnd.at[1])
        sent(BX, xsnd.at[2])
        sent(QT.at[z, 0], xsnd.at[5])
        sent(UN, xsnd.at[4])
        for h in (0, 1):
            sent(PN.at[:, :, :, lanes[h]], xsnd.at[6 + h])
        stored()


def per_device(a, b, c, u, v, p, q):
    dma = pltpu.SemaphoreType.DMA
    anywhere = pl.BlockSpec(memory_space=pltpu.HBM)
    vm = pltpu.VMEM
    scratch = [
        vm((16, 2, 16, 1024), BF16),
        vm((16, 2, 16, 1024), BF16),
        vm((4, 4, 32, 1024), BF16),
        vm((4, 4, 2, 32, 512), BF16),
        vm((4, 4, 32, 512), BF16),
        vm((512, 512), BF16),
        *[vm((512, 1024), BF16) for _ in range(5)],
        vm((16, 32, 1024), F32),
        *[vm((n, 32, 1024), BF16) for n in (4, 4, 3, 3, 4, 4, 4, 4)],
        vm((16, 2, 16, 1024), BF16),
        vm((512, 1024), BF16),
        vm((32, 1024), BF16),
        vm((32, 1024), BF16),
        vm((4, 4, 32, 512), BF16),
        vm((4, 4, 2, 32, 512), F32),
        vm((4, 4, 2, 32, 512), BF16),
        vm((2, 3, 4, 2, 32, HALF), BF16),
        vm((2, 4, 2, 32, HALF), F32),
        vm((2, 4, 2, 32, HALF), BF16),
        vm((2, 3, 2, 32, HALF), BF16),
        vm((4, 4, 2, 32, 512), BF16),
        vm((4, 4, 32, 512), BF16),
        vm((512, 1024), F32),
        dma((7,)), dma((8,)), dma((8,)),
        *[dma((2, 15)), dma((2,)), dma((2, 2))] * 3,
        dma((2, 4)), dma((2, 3)), dma((2, 4)), dma((2, 4)), dma,
        *[dma((4,)), dma((2,))] * 5,
        dma, dma, dma, dma, pltpu.SemaphoreType.REGULAR, pltpu.SemaphoreType.REGULAR, pltpu.SemaphoreType.REGULAR((6,)),
    ]
    return pl.pallas_call(
        kernel,
        out_shape=jax.ShapeDtypeStruct(c.shape, c.dtype),
        in_specs=[anywhere] * 7,
        out_specs=anywhere,
        scratch_shapes=scratch,
        compiler_params=pltpu.CompilerParams(
            collective_id=0, has_side_effects=True, vmem_limit_bytes=67043328
        ),
        name="maintain",
    )(v.T, u.T, p.T, q.T, a, b, c)


def solution(mesh):
    split = Mesh(mesh.devices.reshape(NZ, 2, 4, 4), ("z", "k", "x", "y"))
    row, col = ("z", "k"), ("x", "y")
    placed = (
        P(row, col), P(row, col), P(row, col), P(row, col), P(row, col), P(col, row), P(col, row),
    )
    return jax.shard_map(
        per_device, mesh=split, in_specs=placed, out_specs=P(row, col), check_vma=False
    )
```

```python
import jax
import jax.numpy as jnp
from jax import lax
from jax.experimental import pallas as pl
from jax.experimental.pallas import tpu as pltpu
from jax.sharding import Mesh
from jax.sharding import PartitionSpec as P

MESH = pl.DeviceIdType.MESH
F32 = jnp.float32
BF16 = jnp.bfloat16
NZ = 16
HALF = 256
NT = (((1,), (1,)), ((), ()))
STEPS = (1, 3, 2)


def rem(a, n):
    return lax.rem(a + 2 * n, n)


def kernel(
    vt_h, ut_h, pt_h, qt_h, a_h, b_h, c_h, out_h,
    PT, QT, VT, UU, UN, U, A, AX, B, BX, C, W,
    RSP, RRP, RSM, RRM, LSP, LRP, LSM, LRM, WT,
    OUT, XV, TV, CR, DF, DS, R1, EF, ES, R2, PJ, PN, ACC,
    load_sem, xrcv, xsnd, psem, psnd, pfwd, qsem, qsnd, qfwd, wsem, wsnd, wfwd,
    rpr, rmr, lpr, lmr, rsnd, vsem, vsnd, usem, usnd, crsem, crsnd,
    dsem, dsnd, jsem, jsnd, scsem, scsnd, tvsem, tusnd, free, known, told,
):
    z = lax.axis_index("z")
    k = lax.axis_index("k")
    x = lax.axis_index("x")
    y = lax.axis_index("y")
    sib = {"k": 1 - k}
    zp, zm = {"z": rem(z + 1, NZ)}, {"z": rem(z - 1, NZ)}
    zpp, zmm = {"z": rem(z + 2, NZ)}, {"z": rem(z - 2, NZ)}
    pos = {"x": x, "y": y}
    c = 4 * x + y
    gap = rem(c - z, NZ)
    even = lax.rem(gap, 2) == 0

    def send(src, dst, ssem, rsem, dev):
        pltpu.make_async_remote_copy(
            src_ref=src, dst_ref=dst, send_sem=ssem, recv_sem=rsem,
            device_id=dev, device_id_type=MESH,
        ).start()

    def recv(dst, rsem):
        pltpu.make_async_remote_copy(
            src_ref=dst, dst_ref=dst, send_sem=rsem, recv_sem=rsem,
            device_id=sib, device_id_type=MESH,
        ).wait_recv()

    def sent(ref, ssem):
        pltpu.make_async_remote_copy(
            src_ref=ref, dst_ref=ref, send_sem=ssem, recv_sem=ssem,
            device_id=sib, device_id_type=MESH,
        ).wait_send()

    low, high = pl.ds(0, 512), pl.ds(512, 512)
    own_lanes = pl.ds(pl.multiple_of(512 * k, 512), 512)
    loads = [
        pltpu.make_async_copy(pt_h, PT.at[z, k], load_sem.at[0]),
        pltpu.make_async_copy(vt_h, VT.at[x, y, :, own_lanes], load_sem.at[1]),
        pltpu.make_async_copy(qt_h, QT.at[z, k], load_sem.at[2]),
        pltpu.make_async_copy(ut_h, UU.at[x, y, k], load_sem.at[3]),
        pltpu.make_async_copy(b_h, B, load_sem.at[4]),
        pltpu.make_async_copy(a_h, A, load_sem.at[5]),
        pltpu.make_async_copy(c_h, C, load_sem.at[6]),
    ]
    for copy in loads:
        copy.start()

    barrier = pltpu.get_barrier_semaphore()
    near = [zp, zm, zpp, zmm]
    for axis in ("x", "y"):
        for step in STEPS:
            near.append({axis: rem(pos[axis] + step, 4)})
    peers = [sib] + [{**dev, "k": kk} for dev in near for kk in (0, 1)]
    for dev in peers:
        pl.semaphore_signal(barrier, inc=1, device_id=dev, device_id_type=MESH)
    pl.semaphore_wait(barrier, len(peers))

    class ZWide:
        def __init__(self, buf, rsem, ssem, fwd, part, to={}):
            self.buf, self.rsem, self.ssem, self.fwd, self.part, self.to = buf, rsem, ssem, fwd, part, to

        def at(self, d):
            return self.buf.at[rem(z - d, NZ), self.part]

        def place(self, d):
            return d - 1 if d > 0 else 7 - d

        def out(self, ref, d):
            dev = {1: zp, 2: zpp, -1: zm, -2: zmm}[d if abs(d) < 3 else (2 - d % 2) * (1 if d > 0 else -1)]
            send(ref, ref, self.ssem, self.rsem.at[self.place(d)], {**dev, **self.to})

        def arrive(self, d):
            ref = self.at(d)
            recv(ref, self.rsem.at[self.place(d)])
            return ref

        def share(self, d):
            ref = self.at(d)
            send(ref, ref, self.ssem, self.fwd.at[0 if abs(d) < 6 else 1], sib)

        def start(self):
            self.out(self.at(0), 2)
            self.out(self.at(0), -2)

        def leaves(self, j):
            for sign in (1, -1):
                self.out(self.at(2 * j * sign), (2 * j + 1) * sign)

        def on(self, j):
            for sign, most in ((1, 8), (-1, 7)):
                d = 2 * j * sign
                ref = self.arrive(d)
                if 2 * j + 2 <= most:
                    self.out(ref, d + 2 * sign)

        def off(self, j, skip=False):
            if not skip:
                self.leaves(j - 1)
            if j == 3:
                self.leaves(3)
            self.share(2 * j)
            self.share(-2 * j)

        def leaf(self, j):
            for sign in (1, -1):
                d = (2 * j + 1) * sign
                self.arrive(d)
                self.share(d)

        def last(self):
            self.arrive(8)
            self.share(8)

        def shared(self, group):
            recv(self.buf.at[pl.ds(0, 5 if group else 10), self.part], self.fwd.at[group])

        def done(self):
            sent(self.buf.at[pl.ds(0, 15)], self.ssem)

    class ZNear(ZWide):
        def out(self, ref, d):
            send(ref, ref, self.ssem, self.rsem.at[self.place(d)], zp if d > 0 else zm)

        def start(self):
            self.leaves(0)

        def step(self, s):
            for sign, most in ((1, 8), (-1, 7)):
                if s < most:
                    d = sign * (s + 1)
                    ref = self.arrive(d)
                    if s + 1 < most:
                        self.out(ref, d + sign)
                    self.share(d)

    class PlaneGather:
        def __init__(self, buf, lanes, first, rsem, ssem, base, to):
            self.buf, self.lanes, self.first = buf, lanes, first
            self.rsem, self.ssem, self.base = rsem, ssem, base
            self.mid = (slice(None),) * (len(buf.shape) - 3)
            self.to = to

        def view(self, phase, at):
            if phase == 0:
                spot = {**pos, self.first: at}
                return self.buf.at[(spot["x"], spot["y"], *self.mid, self.lanes)]
            if self.first == "x":
                return self.buf.at[(slice(None), at, *self.mid, self.lanes)]
            return self.buf.at[(at, slice(None), *self.mid, self.lanes)]

        def axis(self, phase):
            return self.first if phase == 0 else ("y" if self.first == "x" else "x")

        def start(self, phase):
            axis = self.axis(phase)
            mine = self.view(phase, pos[axis])
            for step in STEPS:
                dev = {axis: rem(pos[axis] + step, 4), **self.to}
                send(mine, mine, self.ssem.at[phase], self.rsem.at[self.base + phase], dev)

        def wait(self, phase):
            some = (pl.ds(0, 3), slice(None)) if phase else (0, pl.ds(0, 3))
            recv(self.buf.at[(*some, *self.mid, self.lanes)], self.rsem.at[self.base + phase])

    lanes = [pl.ds(0, HALF), pl.ds(HALF, HALF)]
    order = ["x", "y"]

    def halves(buf, rsem, ssem, cut=lanes, to={}):
        return [PlaneGather(buf, cut[h], order[h], rsem, ssem, 2 * h, to) for h in (0, 1)]

    def plane_done(buf, ssem):
        sent(buf.at[0, pl.ds(0, 3)], ssem.at[0])
        sent(buf.at[pl.ds(0, 3)], ssem.at[1])

    gp = [ZWide(PT, psem.at[i], psnd.at[i], pfwd.at[i], i, {"k": 1}) for i in (0, 1)]
    gw = [ZWide(WT, wsem.at[i], wsnd.at[i], wfwd.at[i], i) for i in (0, 1)]
    gq = [ZNear(QT, qsem.at[i], qsnd.at[i], qfwd.at[i], i) for i in (0, 1)]
    gv = halves(VT, vsem, vsnd, [low, high], {"k": 1})
    gu = halves(UU, usem, usnd)
    gc = halves(CR, crsem, crsnd)
    gj = halves(PJ, jsem, jsnd)

    def both(gathers, what, phase):
        for g in gathers:
            getattr(g, what)(phase)

    def tiles(dst, base, left, right):
        for j in range(4):
            at = pl.ds(j * HALF, HALF)
            weights = right[..., at].reshape(512, HALF)
            part = jnp.dot(left, weights, preferred_element_type=F32)
            dst[:, at] = (base[:, at].astype(F32) + part).astype(dst.dtype)
            if dst is OUT:
                result(j).start()

    def result(j):
        at = pl.ds(j * HALF, HALF)
        return pltpu.make_async_copy(OUT.at[:, at], out_h.at[:, at], load_sem.at[j])

    def stored():
        for j in range(4):
            result(j).wait()

    cols = [low, high]

    def rs_out(d, parts, src, dst, rsem, i, p, dev):
        total = W[d, :, cols[p]]
        for ref, sem, n in parts:
            recv(ref.at[n, :, cols[p]], sem.at[p, n])
            total = total + ref[n, :, cols[p]].astype(F32)
        src[i, :, cols[p]] = total.astype(BF16)
        send(src.at[i, :, cols[p]], dst.at[i, :, cols[p]], rsnd, rsem.at[p, i], dev)

    def rs_plus(i, p):
        parts = [(LRP, lpr, i - 1), (RRP, rpr, i - 1)] if i else []
        rs_out(rem(z + 8 - 2 * i, NZ), parts, RSP, RRP, rpr, i, p, zpp)

    def rs_minus(i, p):
        parts = [(LRM, lmr, i)] + ([(RRM, rmr, i - 1)] if i else [])
        rs_out(rem(z - 6 + 2 * i, NZ), parts, RSM, RRM, rmr, i, p, zmm)

    def rs_leaf(i, p):
        rs_out(rem(z - 7 + 2 * i, NZ), [], LSM, LRM, lmr, i, p, zm)
        rs_out(rem(z + 7 - 2 * i, NZ), [], LSP, LRP, lpr, i, p, zp)

    def rs_both(what, i):
        for p in (0, 1):
            what(i, p)

    def sum_w(p):
        left = VT[...].reshape(512, 1024)
        for j in (2 * p, 2 * p + 1):
            at = pl.ds(j * HALF, HALF)
            part = jnp.dot(left[:, :512], BX[:, at], preferred_element_type=F32)
            part = part + jnp.dot(left[:, 512:], B[:, at], preferred_element_type=F32)
            W[:, :, at] = part.reshape(NZ, 32, HALF)

    def cross_part():
        part = lax.dot_general(XV[...], PT[...].reshape(512, 1024), NT, preferred_element_type=F32)
        CR[x, y] = part.astype(BF16)

    def own_w():
        cross = jnp.sum(CR[...].astype(F32).reshape(16, 32, 512), axis=0).astype(BF16)
        total = W[z] + jnp.dot(cross, QT[...].reshape(512, 1024), preferred_element_type=F32)
        for ref, sem, n in ((LRP, lpr, 3), (LRM, lmr, 3), (RRP, rpr, 3), (RRM, rmr, 2)):
            for p in (0, 1):
                recv(ref.at[n, :, cols[p]], sem.at[p, n])
            total = total + ref[n].astype(F32)
        WT[z] = total.astype(BF16).reshape(2, 16, 1024)

    def p_hub(j):
        for g in gp:
            g.on(j)
        gp[0].off(j, j == 1)
        gp[1].off(j)

    def p_leaf(j):
        for g in gp:
            g.leaf(j)

    def w_start():
        for g in gw:
            g.start()

    def w_hub(j):
        for g in gw:
            g.on(j)
        for g in gw:
            g.off(j)

    def w_leaf(j):
        for g in gw:
            g.leaf(j)

    def w_last():
        for g in gw:
            g.last()

    def q_step(s):
        for g in gq:
            g.step(s)

    def tell(i):
        pl.semaphore_signal(told.at[i], inc=1, device_id=zpp, device_id_type=MESH)
        pl.semaphore_signal(told.at[3 + i], inc=1, device_id=zmm, device_id_type=MESH)

    def hear(i):
        pl.semaphore_wait(told.at[i], 1)
        pl.semaphore_wait(told.at[3 + i], 1)

    def scatter():
        def one(d):
            b = rem(z + d, NZ)
            send(VT.at[b // 4, lax.rem(b, 4)], TV, scsnd, tvsem, {"z": b, "k": 1})

        @pl.when(even & (gap != 0))
        def _():
            one(gap // 2)

        @pl.when(even)
        def _():
            one(gap // 2 + 8)

    def turn():
        @pl.when(gap != 0)
        def _():
            recv(TV, tvsem)

        @pl.when(lax.rem(gap, 8) != 0)
        def _():
            a = rem(2 * z - c, NZ)
            send(TV, XV, tusnd, scsem, {"k": 1, "x": a // 4, "y": lax.rem(a, 4)})

        @pl.when(gap == 8)
        def _():
            XV[...] = TV[...]

        @pl.when(gap == 0)
        def _():
            XV[...] = VT[x, y]

    def turned():
        @pl.when(lax.rem(gap, 8) != 0)
        def _():
            recv(XV, scsem)

    @pl.when(k == 1)
    def _():
        loads[1].wait()
        gv[1].start(0)
        loads[0].wait()
        gp[1].start()
        loads[2].wait()
        send(QT.at[z, 1], QT.at[z, 1], xsnd.at[0], xrcv.at[0], sib)
        loads[3].wait()
        send(UU.at[x, y, 1], UU.at[x, y, 1], xsnd.at[1], xrcv.at[1], sib)
        send(PT.at[z, 1], PT.at[z, 1], xsnd.at[5], xrcv.at[5], sib)
        send(a_h, AX, xsnd.at[2], xrcv.at[2], sib)
        gv[1].wait(0)
        gv[1].start(1)
        p_hub(1)
        recv(VT.at[x, y, :, low], xrcv.at[1])
        gv[0].wait(0)
        gv[0].start(1)
        p_hub(2)
        p_leaf(0)
        gv[1].wait(1)
        gv[0].wait(1)
        pl.semaphore_wait(known, 1)

        scatter()

        loads[4].wait()
        recv(BX, xrcv.at[2])
        for p in (0, 1):
            sum_w(p)
            rs_plus(0, p)
            rs_leaf(0, p)
        p_hub(3)
        p_leaf(1)
        rs_both(rs_minus, 0)
        rs_both(rs_leaf, 1)
        rs_both(rs_plus, 1)
        turn()
        rs_both(rs_minus, 1)
        rs_both(rs_leaf, 2)
        p_leaf(2)
        for g in gp:
            g.last()
        p_leaf(3)
        recv(PT.at[z, 0], xrcv.at[0])
        turned()
        cross_part()
        both(gc, "start", 0)
        rs_both(rs_plus, 2)
        both(gc, "wait", 0)
        both(gc, "start", 1)
        rs_both(rs_minus, 2)
        rs_both(rs_leaf, 3)
        rs_both(rs_plus, 3)
        recv(QT.at[z, 0], xrcv.at[5])
        for g in gq:
            g.shared(0)
            g.shared(1)
        both(gc, "wait", 1)
        pl.semaphore_signal(free, inc=1, device_id=sib, device_id_type=MESH)
        own_w()
        w_start()
        send(WT.at[z], WT.at[z], xsnd.at[4], xrcv.at[4], sib)
        w_hub(1)
        w_hub(2)
        w_leaf(0)
        loads[6].wait()
        loads[5].wait()
        recv(UN, xrcv.at[4])
        U[...] = UN[...].reshape(512, 512).T
        w_hub(3)
        w_leaf(1)
        for h in (0, 1):
            recv(PN.at[:, :, :, lanes[h]], xrcv.at[6 + h])
        tiles(ACC, C, PN[...].reshape(512, 512), QT)
        w_leaf(2)
        w_last()
        w_leaf(3)
        tiles(OUT, ACC, U[...], WT)
        sent(PT.at[pl.ds(0, 13)], psnd.at[0])
        for g in (gp[1], *gw):
            g.done()
        sent(PT.at[pl.ds(0, 15)], rsnd)
        sent(VT.at[0, pl.ds(0, 3), :, low], vsnd.at[0])
        sent(VT.at[pl.ds(0, 3)], vsnd.at[1])
        plane_done(CR, crsnd)
        sent(QT.at[z, 1], xsnd.at[0])
        sent(UU.at[x, y, 1], xsnd.at[1])
        sent(AX, xsnd.at[2])
        sent(WT.at[z], xsnd.at[4])
        sent(PT.at[z, 1], xsnd.at[5])

        @pl.when(even & (gap != 0))
        def _():
            sent(PT.at[pl.ds(0, 2)], scsnd)

        @pl.when(gap == 0)
        def _():
            sent(PT.at[0], scsnd)

        @pl.when(lax.rem(gap, 8) != 0)
        def _():
            sent(TV, tusnd)

        stored()


    def d_part(h):
        points = PT[pl.ds(8 * h, 8)].reshape(HALF, 1024)
        for r, left in ((0, A), (1, AX)):
            part = lax.dot_general(left[...], points, NT, preferred_element_type=F32).reshape(4, 4, 32, HALF)
            DF[:, :, r, :, lanes[h]] = part
            DS[:, :, r, :, lanes[h]] = part.astype(BF16)

    def d_start(h, phase):
        axis = order[h] if phase == 0 else order[1 - h]
        for i, step in enumerate(STEPS):
            t = rem(pos[axis] + step, 4)
            if phase == 1:
                src, dst = ES.at[h, t], R2.at[h, i]
            else:
                src = DS.at[t, :, :, :, lanes[h]] if h == 0 else DS.at[:, t, :, :, lanes[h]]
                dst = R1.at[h, i]
            send(src, dst, dsnd.at[phase], dsem.at[2 * h + phase], {axis: t})

    def d_first(h):
        recv(R1.at[h], dsem.at[2 * h])
        total = DF[x, :, :, :, lanes[h]] if h == 0 else DF[:, y, :, :, lanes[h]]
        for i in range(3):
            total = total + R1[h, i].astype(F32)
        EF[h] = total
        ES[h] = total.astype(BF16)
        d_start(h, 1)

    def d_second(h):
        recv(R2.at[h], dsem.at[2 * h + 1])
        total = EF[h, pos[order[1 - h]]]
        for i in range(3):
            total = total + R2[h, i].astype(F32)
        PJ[x, y, :, :, lanes[h]] = total.astype(BF16)

    @pl.when(k == 0)
    def _():
        tell(0)
        loads[1].wait()
        gv[0].start(0)
        loads[0].wait()
        gp[0].start()
        send(VT.at[x, y, :, low], VT.at[x, y, :, low], xsnd.at[1], xrcv.at[1], sib)
        loads[2].wait()
        gq[0].start()
        recv(QT.at[z, 1], xrcv.at[0])
        gq[1].start()
        gp[0].leaves(0)
        send(b_h, BX, xsnd.at[2], xrcv.at[2], sib)
        send(PT.at[z, 0], PT.at[z, 0], xsnd.at[0], xrcv.at[0], sib)
        send(QT.at[z, 0], QT.at[z, 0], xsnd.at[5], xrcv.at[5], sib)
        loads[3].wait()
        recv(UU.at[x, y, 1], xrcv.at[1])
        hear(0)
        tell(1)
        q_step(0)
        both(gu, "start", 0)
        hear(1)
        tell(2)
        q_step(1)
        hear(2)
        pl.semaphore_signal(known, inc=1, device_id=sib, device_id_type=MESH)
        q_step(2)
        both(gu, "wait", 0)
        both(gu, "start", 1)
        q_step(3)

        q_step(4)
        recv(PT.at[z, 1], xrcv.at[5])
        for g in gp:
            g.shared(0)
            g.shared(1)
        loads[5].wait()
        recv(AX, xrcv.at[2])
        d_part(0)
        d_start(0, 0)
        d_part(1)
        d_start(1, 0)
        q_step(5)
        q_step(6)
        d_first(0)
        d_first(1)
        q_step(7)
        d_second(0)
        d_second(1)
        pl.semaphore_wait(free, 1)
        both(gj, "start", 0)
        both(gu, "wait", 1)
        send(UU.at[:, :, 1], UN, xsnd.at[4], xrcv.at[4], sib)
        for g in gj:
            g.wait(0)
            g.start(1)
        U[...] = UU[:, :, 0].reshape(512, 512).T
        loads[6].wait()
        loads[4].wait()
        for h in (0, 1):
            gj[h].wait(1)
            send(PJ.at[:, :, 1, :, lanes[h]], PN.at[:, :, :, lanes[h]], xsnd.at[6 + h], xrcv.at[6 + h], sib)
        tiles(ACC, C, PJ[:, :, 0].reshape(512, 512), QT)
        recv(WT.at[z], xrcv.at[4])
        for g in gw:
            g.shared(0)
        for g in gw:
            g.shared(1)
        tiles(OUT, ACC, U[...], WT)
        for g in gq:
            g.done()
        sent(PT.at[pl.ds(0, 2)], psnd.at[0])
        sent(VT.at[0, pl.ds(0, 3), :, low], vsnd.at[0])
        plane_done(UU, usnd)
        plane_done(PJ, jsnd)
        sent(R1, dsnd.at[0])
        sent(R2, dsnd.at[1])
        sent(PT.at[z, 0], xsnd.at[0])
        sent(VT.at[x, y, :, low], xsnd.at[1])
        sent(BX, xsnd.at[2])
        sent(QT.at[z, 0], xsnd.at[5])
        sent(UN, xsnd.at[4])
        for h in (0, 1):
            sent(PN.at[:, :, :, lanes[h]], xsnd.at[6 + h])
        stored()


def per_device(a, b, c, u, v, p, q):
    dma = pltpu.SemaphoreType.DMA
    anywhere = pl.BlockSpec(memory_space=pltpu.HBM)
    vm = pltpu.VMEM
    scratch = [
        vm((16, 2, 16, 1024), BF16),
        vm((16, 2, 16, 1024), BF16),
        vm((4, 4, 32, 1024), BF16),
        vm((4, 4, 2, 32, 512), BF16),
        vm((4, 4, 32, 512), BF16),
        vm((512, 512), BF16),
        *[vm((512, 1024), BF16) for _ in range(5)],
        vm((16, 32, 1024), F32),
        *[vm((n, 32, 1024), BF16) for n in (4, 4, 3, 3, 4, 4, 4, 4)],
        vm((16, 2, 16, 1024), BF16),
        vm((512, 1024), BF16),
        vm((32, 1024), BF16),
        vm((32, 1024), BF16),
        vm((4, 4, 32, 512), BF16),
        vm((4, 4, 2, 32, 512), F32),
        vm((4, 4, 2, 32, 512), BF16),
        vm((2, 3, 4, 2, 32, HALF), BF16),
        vm((2, 4, 2, 32, HALF), F32),
        vm((2, 4, 2, 32, HALF), BF16),
        vm((2, 3, 2, 32, HALF), BF16),
        vm((4, 4, 2, 32, 512), BF16),
        vm((4, 4, 32, 512), BF16),
        vm((512, 1024), F32),
        dma((7,)), dma((8,)), dma((8,)),
        *[dma((2, 15)), dma((2,)), dma((2, 2))] * 3,
        dma((2, 4)), dma((2, 3)), dma((2, 4)), dma((2, 4)), dma,
        *[dma((4,)), dma((2,))] * 5,
        dma, dma, dma, dma, pltpu.SemaphoreType.REGULAR, pltpu.SemaphoreType.REGULAR, pltpu.SemaphoreType.REGULAR((6,)),
    ]
    return pl.pallas_call(
        kernel,
        out_shape=jax.ShapeDtypeStruct(c.shape, c.dtype),
        in_specs=[anywhere] * 7,
        out_specs=anywhere,
        scratch_shapes=scratch,
        compiler_params=pltpu.CompilerParams(
            collective_id=0, has_side_effects=True, vmem_limit_bytes=67043328
        ),
        name="maintain",
    )(v.T, u.T, p.T, q.T, a, b, c)


def solution(mesh):
    split = Mesh(mesh.devices.reshape(NZ, 2, 4, 4), ("z", "k", "x", "y"))
    row, col = ("z", "k"), ("x", "y")
    placed = (
        P(row, col), P(row, col), P(row, col), P(row, col), P(row, col), P(col, row), P(col, row),
    )
    return jax.shard_map(
        per_device, mesh=split, in_specs=placed, out_specs=P(row, col), check_vma=False
    )
```
